128 devices in a mesh: gx: 16 (over x, z), gy: 8 (over y, core).
Axes of the slice: x: 4, y: 4, z: 4, core: 2. Of those that a mesh axis runs over, the one named last changes fastest.
Arguments:
- source_tiles: bfloat16 [384, 32, 192, 384], P(('gx', 'gy')), may hold values from -6 to 6
- tile_offsets: int32 [2, 384], P(None, ('gx', 'gy')), may hold values from -128 to 1920, as said below
- tile_shifts: int32 [384], P(('gx', 'gy')), may hold values from 0 to 63
- tile_counts: int32 [128], P(('gx', 'gy')), may hold values from 1 to 3, as said below
Outputs:
- merged_slab: float32 [32, 2048, 2048], P(None, 'gx', 'gy')
The draws below stay inside these ranges and needn't reach their ends.
Inputs may be any that keep to these rules, and one draw needn't show every extreme that they name: `tile_offsets`: slot k belongs to the device of joined gx+gy index d = k // 3, that is gx index d // 8 and gy index d % 8. Its x offset lies from that gx index times 128 minus 64 up to that gx index times 128; its y offset from the gy index times 256 minus 128 up to the gy index times 256. So every tile covers its owner's whole block. `tile_counts`: entry d counts the used slots of device d; they are its first slots, the others are ignored. Both 1 and 3 occur in every draw.
All inputs are finite; a program needn't handle non-finite values.
Results may differ from the reference program's by a relative error of at most 0.0003.
Values sent between devices are 32-bit elements; how exact they have to be, the bound alone decides.
A program may use at most 192 MiB of HBM per device.

```python
import jax
import jax.numpy as jnp
from jax import lax

NZ = 32
BX = 128
BY = 256
TX = 192
TY = 384
CAP = 3
RAMP = 32
NSHIFT = 64
RX = 64
RY = 128
NX = 2048
NY = 2048
TILES = 384


def draw_tile_offsets(key, part):
    holders = jnp.arange(TILES, dtype=jnp.int32) // CAP
    rows_gy = NY // BY
    column = holders // rows_gy
    row_place = holders % rows_gy
    key_x, key_y = jax.random.split(jax.random.fold_in(key, 11))
    back_x = jax.random.randint(key_x, (TILES,), 0, TX - BX + 1)
    back_y = jax.random.randint(key_y, (TILES,), 0, TY - BY + 1)
    back_x = back_x.at[0].set(TX - BX).at[TILES - 1].set(0)
    back_y = back_y.at[0].set(TY - BY).at[TILES - 1].set(0)
    return jnp.stack([column * BX - back_x, row_place * BY - back_y]).astype(jnp.int32)


def draw_tile_counts(key, part):
    counts = jax.random.randint(jax.random.fold_in(key, 23), (TILES // CAP,), 1, CAP + 1)
    counts = counts.at[0].set(CAP).at[1].set(1)
    return counts.astype(jnp.int32)


def plant(array, stream_key, smallest, top_value):
    longest = array.shape.index(max(array.shape))
    spots = []
    for shift in (0, 1):
        where = [jax.random.randint(jax.random.fold_in(stream_key, axis), (), 0, length) for axis, length in enumerate(array.shape)]
        where[longest] = (where[longest] + shift) % array.shape[longest]
        spots.append(tuple(where))
    return array.at[spots[0]].set(smallest).at[spots[1]].set(top_value)


def block_scale(rng, extent, shards, least, top_value):
    loudness = 1.0
    for dim, parts in shards:
        draws = jax.random.uniform(jax.random.fold_in(jax.random.fold_in(rng, 6), dim), (parts,), jnp.float32, least / len(shards), top_value / len(shards))
        loudness = loudness * jnp.repeat(jnp.exp(draws), extent[dim] // parts).reshape((-1,) + (1,) * (len(extent) - 1 - dim))
    return loudness


def noise(rng, extent, scale, bound, shards=(), kind=jnp.bfloat16):
    entries = scale * jax.random.normal(rng, extent, jnp.float32)
    if shards:
        entries = entries * block_scale(rng, extent, shards, -0.22, 0.18)
    return jnp.clip(entries, -bound, bound).astype(kind)


def setup_inputs(seed: int = 0) -> dict:
    streams_of = jax.random.split(jax.random.key(seed), 5)
    return {
        "source_tiles": noise(streams_of[0], (TILES, NZ, TX, TY), 1.0, 6.0, ((0, 128),)),
        "tile_offsets": draw_tile_offsets(jax.random.fold_in(streams_of[4], 71), 0),
        "tile_shifts": plant(jax.random.randint(streams_of[2], (TILES,), 0, NSHIFT), jax.random.fold_in(streams_of[2], 1), 0, NSHIFT - 1).astype(jnp.int32),
        "tile_counts": draw_tile_counts(jax.random.fold_in(streams_of[4], 71), 0),
    }


def interpolate(volume, fraction, dimension):
    length = volume.shape[dimension]
    shifted = jnp.concatenate([lax.slice_in_dim(volume, 1, length, axis=dimension), lax.slice_in_dim(volume, length - 1, length, axis=dimension)], axis=dimension)
    return (1.0 - fraction) * volume + fraction * shifted


def resample(source, shift_code):
    depth_part = ((shift_code // 16) % 4).astype(jnp.float32) * 0.25
    column_part = ((shift_code // 4) % 4).astype(jnp.float32) * 0.25
    row_part = (shift_code % 4).astype(jnp.float32) * 0.25
    volume = source.astype(jnp.float32)
    volume = interpolate(volume, depth_part, 0)
    volume = interpolate(volume, column_part, 1)
    return interpolate(volume, row_part, 2)


def blend_ramp(length):
    places = jnp.arange(length, dtype=jnp.float32)
    return jnp.minimum(jnp.minimum(places + 1.0, length - places), float(RAMP))


def reference(source_tiles, tile_offsets, tile_shifts, tile_counts):
    weight_plane = blend_ramp(TX)[:, None] * blend_ramp(TY)[None, :]
    values = jnp.zeros((NZ, NX + 2 * RX, NY + 2 * RY), jnp.float32)
    weights = jnp.zeros((NX + 2 * RX, NY + 2 * RY), jnp.float32)

    def place_tile(accumulated, number):
        values, weights = accumulated
        holder = number // CAP
        active = ((number % CAP) < tile_counts[holder]).astype(jnp.float32)
        source = lax.dynamic_index_in_dim(source_tiles, number, 0, keepdims=False)
        scaled = active * weight_plane
        volume = resample(source, tile_shifts[number]) * scaled[None]
        start_x = (tile_offsets[0, number] + RX).astype(jnp.int32)
        start_y = (tile_offsets[1, number] + RY).astype(jnp.int32)
        anchor = jnp.int32(0)
        window = lax.dynamic_slice(values, (anchor, start_x, start_y), (NZ, TX, TY))
        values = lax.dynamic_update_slice(values, window + volume, (anchor, start_x, start_y))
        weight_window = lax.dynamic_slice(weights, (start_x, start_y), (TX, TY))
        weights = lax.dynamic_update_slice(weights, weight_window + scaled, (start_x, start_y))
        return (values, weights), None

    (values, weights), ignored = lax.scan(place_tile, (values, weights), jnp.arange(TILES, dtype=jnp.int32))
    block_weights = weights[RX:RX + NX, RY:RY + NY]
    return values[:, RX:RX + NX, RY:RY + NY] / jnp.maximum(block_weights, 1.0)[None]
```

```python
import jax
import jax.numpy as jnp
from jax import lax
from jax.experimental import pallas as pl
from jax.experimental.pallas import tpu as pltpu
from jax.sharding import PartitionSpec as P

NZ = 32
BX = 128
BY = 256
TX = 192
TY = 384
CAP = 3
RAMP = 32
RX = 64
RY = 128
WX = BX + 2 * RX
WY = BY + 2 * RY
SLOTS = NZ + 1
LAG_Y = 2
LAG_X = 4
ROWS = 16
MESH = pl.DeviceIdType.MESH


def ramp(places, length):
    return jnp.minimum(jnp.minimum(places + 1, length - places), RAMP)


def taps(places, length, fraction):
    inside = (places >= 0) & (places < length)
    blend = jnp.where(inside, ramp(places, length), 0).astype(jnp.float32)
    last = jnp.where(places == length - 1, fraction, 0.0)
    return blend, blend * (1.0 - fraction + last), blend * fraction


def kernel(
    tiles, offsets, shifts, counts, out,
    source, edge_low, edge_high, block, from_low, from_high, from_left, from_right,
    mid, split, spread_y, spread_x, inverse,
    load_sem, store_sem, send_low, send_high, send_left, send_right,
    recv_low, recv_high, recv_left, recv_right,
):
    gx = lax.axis_index("gx")
    gy = lax.axis_index("gy")
    last_x = lax.axis_size("gx") - 1
    last_y = lax.axis_size("gy") - 1
    has_low, has_high = gy > 0, gy < last_y
    has_left, has_right = gx > 0, gx < last_x

    def load(z):
        return pltpu.make_async_copy(tiles.at[:, z], source.at[:, z], load_sem.at[z])

    def store(z):
        return pltpu.make_async_copy(
            block.at[z + 1, pl.ds(RX, BX)], out.at[z], store_sem.at[z]
        )

    def to_low(slot):
        return pltpu.make_async_remote_copy(
            src_ref=edge_low.at[slot], dst_ref=from_high.at[slot],
            send_sem=send_low.at[slot], recv_sem=recv_high.at[slot],
            device_id={"gy": gy - 1}, device_id_type=MESH,
        )

    def to_high(slot):
        return pltpu.make_async_remote_copy(
            src_ref=edge_high.at[slot], dst_ref=from_low.at[slot],
            send_sem=send_high.at[slot], recv_sem=recv_low.at[slot],
            device_id={"gy": gy + 1}, device_id_type=MESH,
        )

    def to_left(slot):
        return pltpu.make_async_remote_copy(
            src_ref=block.at[slot, pl.ds(0, RX)], dst_ref=from_right.at[slot],
            send_sem=send_left.at[slot], recv_sem=recv_right.at[slot],
            device_id={"gx": gx - 1}, device_id_type=MESH,
        )

    def to_right(slot):
        return pltpu.make_async_remote_copy(
            src_ref=block.at[slot, pl.ds(RX + BX, RX)], dst_ref=from_left.at[slot],
            send_sem=send_right.at[slot], recv_sem=recv_left.at[slot],
            device_id={"gx": gx + 1}, device_id_type=MESH,
        )

    load(0).start()
    load(1).start()

    barrier = pltpu.get_barrier_semaphore()
    for present, place in (
        (has_low, {"gy": gy - 1}), (has_high, {"gy": gy + 1}),
        (has_left, {"gx": gx - 1}), (has_right, {"gx": gx + 1}),
    ):
        @pl.when(present)
        def _(place=place):
            pl.semaphore_signal(barrier, inc=1, device_id=place, device_id_type=MESH)

    def start_y(slot):
        @pl.when(has_low)
        def _():
            to_low(slot).start()

        @pl.when(has_high)
        def _():
            to_high(slot).start()

    starts_x, starts_y, parts, used = [], [], [], []
    for k in range(CAP):
        code = shifts[k]
        starts_x.append(offsets[0, k] - gx * BX + RX)
        starts_y.append(offsets[1, k] - gy * BY + RY)
        parts.append([
            ((code >> bits) & 3).astype(jnp.float32) * 0.25 for bits in (4, 2, 0)
        ])
        used.append(jnp.where(k < counts[0], 1.0, 0.0).astype(jnp.float32))

    rows_x = lax.broadcasted_iota(jnp.int32, (WX, 128), 0)
    cells_y = lax.broadcasted_iota(jnp.int32, (8, WY), 1)
    plane_y, taps_y, total = [], [], []
    for k in range(CAP):
        taps_y.append(taps(cells_y - starts_y[k], TY, parts[k][2]))
    for n in range(WY // 128):
        total = jnp.zeros((WX, 128), jnp.float32)
        for k in range(CAP):
            blend_x = taps(rows_x - starts_x[k], TX, parts[k][1])[0] * used[k]
            total = total + blend_x * taps_y[k][0][0:1, n * 128 : (n + 1) * 128]
        if n == 0:
            edge_low[0] = total
        elif n == WY // 128 - 1:
            edge_high[0] = total
        else:
            block[0, :, (n - 1) * 128 : n * 128] = total

    pl.semaphore_wait(
        barrier,
        has_low.astype(jnp.int32) + has_high.astype(jnp.int32)
        + has_left.astype(jnp.int32) + has_right.astype(jnp.int32),
    )
    start_y(0)

    def start_load(z, carry):
        load(z).start()
        return carry

    lax.fori_loop(2, NZ, start_load, 0)

    for k in range(CAP):
        for r in range(0, TY, 64):
            apart = (
                lax.broadcasted_iota(jnp.int32, (64, WY), 0) + r
                - lax.broadcasted_iota(jnp.int32, (64, WY), 1) + starts_y[k]
            )
            here, after = taps_y[k][1][0:1], taps_y[k][2][0:1]
            spread_y[k, r : r + 64] = jnp.where(
                apart == 0, here, jnp.where(apart == 1, after, 0.0)
            ).astype(jnp.bfloat16)
        lane = lax.broadcasted_iota(jnp.int32, (64, 2 * TX), 1)
        lane = jnp.where(lane >= TX, lane - TX, lane)
        for r in range(0, WX, 64):
            place = lax.broadcasted_iota(jnp.int32, (64, 2 * TX), 0) + r - starts_x[k]
            _, here, after = taps(place, TX, parts[k][1])
            apart = lane - place
            spread_x[r : r + 64, k * 2 * TX : (k + 1) * 2 * TX] = (
                jnp.where(apart == 0, here, jnp.where(apart == 1, after, 0.0)) * used[k]
            ).astype(jnp.bfloat16)

    def along_y(z):
        load(z).wait()
        for k in range(CAP):
            mid[z % 2, k] = jnp.dot(
                source[k, z], spread_y[k], preferred_element_type=jnp.float32
            )

    along_y(0)

    def step(slot, carry):
        @pl.when(slot < SLOTS)
        def _():
            z = slot - 1

            @pl.when(z < NZ - 1)
            def _():
                along_y(z + 1)

            now = z % 2
            then = jnp.minimum(z + 1, NZ - 1) % 2
            for k in range(CAP):
                depth_part = parts[k][0]
                for r in range(0, TX, ROWS):
                    volume = (1.0 - depth_part) * mid[now, k, r : r + ROWS] + (
                        depth_part * mid[then, k, r : r + ROWS]
                    )
                    coarse = volume.astype(jnp.bfloat16)
                    fine = (volume - coarse.astype(jnp.float32)).astype(jnp.bfloat16)
                    split[k * 2 * TX + r : k * 2 * TX + r + ROWS] = coarse
                    split[k * 2 * TX + TX + r : k * 2 * TX + TX + r + ROWS] = fine
            for n in range(2):
                piece = jnp.dot(
                    spread_x[...], split[:, n * 256 : (n + 1) * 256],
                    preferred_element_type=jnp.float32,
                )
                if n == 0:
                    edge_low[slot] = piece[:, :128]
                    block[slot, :, :128] = piece[:, 128:]
                else:
                    block[slot, :, 128:] = piece[:, :128]
                    edge_high[slot] = piece[:, 128:]
            start_y(slot)

        ready = slot - LAG_Y

        @pl.when((ready >= 0) & (ready < SLOTS))
        def _():
            @pl.when(has_low)
            def _():
                to_high(ready).wait_recv()
                block[ready, :, :RY] += from_low[ready]

            @pl.when(has_high)
            def _():
                to_low(ready).wait_recv()
                block[ready, :, RY:] += from_high[ready]

            @pl.when(has_left)
            def _():
                to_left(ready).start()

            @pl.when(has_right)
            def _():
                to_right(ready).start()

        done = slot - LAG_X

        @pl.when((done >= 0) & (done < SLOTS))
        def _():
            @pl.when(has_left)
            def _():
                to_right(done).wait_recv()
                block[done, RX : 2 * RX] += from_left[done]

            @pl.when(has_right)
            def _():
                to_left(done).wait_recv()
                block[done, 2 * RX : 3 * RX] += from_right[done]

            @pl.when(done == 0)
            def _():
                inverse[...] = 1.0 / jnp.maximum(block[0, RX : RX + BX], 1.0)

            @pl.when(done > 0)
            def _():
                block[done, RX : RX + BX] *= inverse[...]
                store(done - 1).start()

        return carry

    lax.fori_loop(1, SLOTS + LAG_X, step, 0)

    def finish(slot, carry):
        @pl.when(has_low)
        def _():
            to_low(slot).wait_send()

        @pl.when(has_high)
        def _():
            to_high(slot).wait_send()

        @pl.when(has_left)
        def _():
            to_left(slot).wait_send()

        @pl.when(has_right)
        def _():
            to_right(slot).wait_send()

        @pl.when(slot < NZ)
        def _():
            store(slot).wait()

        return carry

    lax.fori_loop(0, SLOTS, finish, 0)


def local(source_tiles, tile_offsets, tile_shifts, tile_counts):
    hbm = pl.BlockSpec(memory_space=pl.ANY)
    smem = pl.BlockSpec(memory_space=pltpu.SMEM)
    dma = pltpu.SemaphoreType.DMA
    return pl.pallas_call(
        kernel,
        out_shape=jax.ShapeDtypeStruct((NZ, BX, BY), jnp.float32),
        in_specs=[hbm, smem, smem, smem],
        out_specs=hbm,
        scratch_shapes=[
            pltpu.VMEM((CAP, NZ, TX, TY), jnp.bfloat16),
            pltpu.VMEM((SLOTS, WX, RY), jnp.float32),
            pltpu.VMEM((SLOTS, WX, RY), jnp.float32),
            pltpu.VMEM((SLOTS, WX, BY), jnp.float32),
            pltpu.VMEM((SLOTS, WX, RY), jnp.float32),
            pltpu.VMEM((SLOTS, WX, RY), jnp.float32),
            pltpu.VMEM((SLOTS, RX, BY), jnp.float32),
            pltpu.VMEM((SLOTS, RX, BY), jnp.float32),
            pltpu.VMEM((2, CAP, TX, WY), jnp.float32),
            pltpu.VMEM((CAP * 2 * TX, WY), jnp.bfloat16),
            pltpu.VMEM((CAP, TY, WY), jnp.bfloat16),
            pltpu.VMEM((WX, CAP * 2 * TX), jnp.bfloat16),
            pltpu.VMEM((BX, BY), jnp.float32),
            dma((NZ,)), dma((NZ,)),
            dma((SLOTS,)), dma((SLOTS,)), dma((SLOTS,)), dma((SLOTS,)),
            dma((SLOTS,)), dma((SLOTS,)), dma((SLOTS,)), dma((SLOTS,)),
        ],
        compiler_params=pltpu.CompilerParams(
            collective_id=0, has_side_effects=True, vmem_limit_bytes=62 * 1024 * 1024,
        ),
    )(source_tiles, tile_offsets, tile_shifts, tile_counts)


def solution(mesh):
    placed = (
        P(("gx", "gy"), None, None, None),
        P(None, ("gx", "gy")),
        P(("gx", "gy")),
        P(("gx", "gy")),
    )
    return jax.shard_map(
        local, mesh=mesh, in_specs=placed, out_specs=P(None, "gx", "gy"), check_vma=False
    )
```

```python
import jax
import jax.numpy as jnp
from jax import lax
from jax.experimental import pallas as pl
from jax.experimental.pallas import tpu as pltpu
from jax.sharding import PartitionSpec as P

NZ = 32
BX = 128
BY = 256
TX = 192
TY = 384
CAP = 3
RAMP = 32
RX = 64
RY = 128
WX = BX + 2 * RX
WY = BY + 2 * RY
SLOTS = NZ
LAG_Y = 3
LAG_X = 8
ROWS = 16
MESH = pl.DeviceIdType.MESH


def ramp(places, length):
    return jnp.minimum(jnp.minimum(places + 1, length - places), RAMP)


def taps(places, length, fraction):
    inside = (places >= 0) & (places < length)
    blend = jnp.where(inside, ramp(places, length), 0).astype(jnp.float32)
    last = jnp.where(places == length - 1, fraction, 0.0)
    return blend, blend * (1.0 - fraction + last), blend * fraction


def kernel(
    tiles, offsets, shifts, counts, out,
    source, edge_low, edge_high, block, from_low, from_high, from_left, from_right,
    mid, split, spread_y, spread_x, inverse,
    ramps, ramps_from_low, ramps_from_high, around, around_left, around_right,
    load_sem, ramp_sem, send_low, send_high, send_left, send_right,
    recv_low, recv_high, recv_left, recv_right,
):
    gx = lax.axis_index("gx")
    gy = lax.axis_index("gy")
    last_x = lax.axis_size("gx") - 1
    last_y = lax.axis_size("gy") - 1
    has_low, has_high = gy > 0, gy < last_y
    has_left, has_right = gx > 0, gx < last_x

    def load(z):
        return pltpu.make_async_copy(tiles.at[:, z], source.at[:, z], load_sem.at[z])

    def to_low(slot):
        return pltpu.make_async_remote_copy(
            src_ref=edge_low.at[slot], dst_ref=from_high.at[slot],
            send_sem=send_low.at[slot], recv_sem=recv_high.at[slot],
            device_id={"gy": gy - 1}, device_id_type=MESH,
        )

    def to_high(slot):
        return pltpu.make_async_remote_copy(
            src_ref=edge_high.at[slot], dst_ref=from_low.at[slot],
            send_sem=send_high.at[slot], recv_sem=recv_low.at[slot],
            device_id={"gy": gy + 1}, device_id_type=MESH,
        )

    def to_left(slot):
        return pltpu.make_async_remote_copy(
            src_ref=block.at[slot, pl.ds(0, RX)], dst_ref=from_right.at[slot],
            send_sem=send_left.at[slot], recv_sem=recv_right.at[slot],
            device_id={"gx": gx - 1}, device_id_type=MESH,
        )

    def to_right(slot):
        return pltpu.make_async_remote_copy(
            src_ref=block.at[slot, pl.ds(RX + BX, RX)], dst_ref=from_left.at[slot],
            send_sem=send_right.at[slot], recv_sem=recv_left.at[slot],
            device_id={"gx": gx + 1}, device_id_type=MESH,
        )

    def ramps_low():
        return pltpu.make_async_remote_copy(
            src_ref=ramps, dst_ref=ramps_from_high,
            send_sem=ramp_sem.at[0], recv_sem=ramp_sem.at[4],
            device_id={"gy": gy - 1}, device_id_type=MESH,
        )

    def ramps_high():
        return pltpu.make_async_remote_copy(
            src_ref=ramps, dst_ref=ramps_from_low,
            send_sem=ramp_sem.at[1], recv_sem=ramp_sem.at[5],
            device_id={"gy": gy + 1}, device_id_type=MESH,
        )

    def ramps_left():
        return pltpu.make_async_remote_copy(
            src_ref=around, dst_ref=around_right,
            send_sem=ramp_sem.at[2], recv_sem=ramp_sem.at[6],
            device_id={"gx": gx - 1}, device_id_type=MESH,
        )

    def ramps_right():
        return pltpu.make_async_remote_copy(
            src_ref=around, dst_ref=around_left,
            send_sem=ramp_sem.at[3], recv_sem=ramp_sem.at[7],
            device_id={"gx": gx + 1}, device_id_type=MESH,
        )

    for z in range(4):
        load(z).start()

    barrier = pltpu.get_barrier_semaphore()
    for present, place in (
        (has_low, {"gy": gy - 1}), (has_high, {"gy": gy + 1}),
        (has_left, {"gx": gx - 1}), (has_right, {"gx": gx + 1}),
    ):
        @pl.when(present)
        def _(place=place):
            pl.semaphore_signal(barrier, inc=1, device_id=place, device_id_type=MESH)

    def start_y(slot):
        @pl.when(has_low)
        def _():
            to_low(slot).start()

        @pl.when(has_high)
        def _():
            to_high(slot).start()

    starts_x, starts_y, parts, used = [], [], [], []
    for k in range(CAP):
        code = shifts[k]
        starts_x.append(offsets[0, k] - gx * BX + RX)
        starts_y.append(offsets[1, k] - gy * BY + RY)
        parts.append([
            ((code >> bits) & 3).astype(jnp.float32) * 0.25 for bits in (4, 2, 0)
        ])
        used.append(jnp.where(k < counts[0], 1.0, 0.0).astype(jnp.float32))

    taps_y = [
        taps(lax.broadcasted_iota(jnp.int32, (8, WY), 1) - starts_y[k], TY, parts[k][2])
        for k in range(CAP)
    ]
    taps_x = [
        taps(lax.broadcasted_iota(jnp.int32, (8, WX), 1) - starts_x[k], TX, parts[k][1])
        for k in range(CAP)
    ]
    ramps[...] = jnp.zeros_like(ramps)
    for k in range(CAP):
        ramps[k : k + 1, :WX] = taps_x[k][0][0:1] * used[k]
        ramps[k : k + 1, WX:] = taps_y[k][0][0:1]

    def start_load(z, carry):
        load(z).start()
        return carry

    lax.fori_loop(4, NZ, start_load, 0)

    for k in range(CAP):
        for r in range(0, TY, 64):
            apart = (
                lax.broadcasted_iota(jnp.int32, (64, WY), 0) + r
                - lax.broadcasted_iota(jnp.int32, (64, WY), 1) + starts_y[k]
            )
            here, after = taps_y[k][1][0:1], taps_y[k][2][0:1]
            spread_y[k, r : r + 64] = jnp.where(
                apart == 0, here, jnp.where(apart == 1, after, 0.0)
            ).astype(jnp.bfloat16)
        lane = lax.broadcasted_iota(jnp.int32, (64, 2 * TX), 1)
        lane = jnp.where(lane >= TX, lane - TX, lane)
        for r in range(0, WX, 64):
            place = lax.broadcasted_iota(jnp.int32, (64, 2 * TX), 0) + r - starts_x[k]
            _, here, after = taps(place, TX, parts[k][1])
            apart = lane - place
            spread_x[r : r + 64, k * 2 * TX : (k + 1) * 2 * TX] = (
                jnp.where(apart == 0, here, jnp.where(apart == 1, after, 0.0)) * used[k]
            ).astype(jnp.bfloat16)

    def along_y(z):
        load(z).wait()
        for k in range(CAP):
            mid[z % 2, k] = jnp.dot(
                source[k, z], spread_y[k], preferred_element_type=jnp.float32
            )

    def resample_x(z):
        now = z % 2
        then = jnp.minimum(z + 1, NZ - 1) % 2
        for k in range(CAP):
            depth_part = parts[k][0]
            for r in range(0, TX, ROWS):
                volume = (1.0 - depth_part) * mid[now, k, r : r + ROWS] + (
                    depth_part * mid[then, k, r : r + ROWS]
                )
                coarse = volume.astype(jnp.bfloat16)
                fine = (volume - coarse.astype(jnp.float32)).astype(jnp.bfloat16)
                split[k * 2 * TX + r : k * 2 * TX + r + ROWS] = coarse
                split[k * 2 * TX + TX + r : k * 2 * TX + TX + r + ROWS] = fine
        for n in range(2):
            piece = jnp.dot(
                spread_x[...], split[:, n * 256 : (n + 1) * 256],
                preferred_element_type=jnp.float32,
            )
            if n == 0:
                edge_low[z] = piece[:, :128]
                block[z, :, :128] = piece[:, 128:]
            else:
                block[z, :, 128:] = piece[:, :128]
                edge_high[z] = piece[:, 128:]

    along_y(0)
    along_y(1)
    resample_x(0)

    pl.semaphore_wait(
        barrier,
        has_low.astype(jnp.int32) + has_high.astype(jnp.int32)
        + has_left.astype(jnp.int32) + has_right.astype(jnp.int32),
    )
    start_y(0)

    @pl.when(has_low)
    def _():
        ramps_low().start()

    @pl.when(has_high)
    def _():
        ramps_high().start()

    def gather_ramps():
        around[...] = jnp.zeros_like(around)
        around[0:8, :WX] = ramps[:, :WX]
        around[0:8, WX:] = ramps[:, WX + RY : WX + RY + BY]

        @pl.when(has_low)
        def _():
            ramps_high().wait_recv()
            around[8:16, :WX] = ramps_from_low[:, :WX]
            around[8:16, WX : WX + RY] = ramps_from_low[:, WX + RY + BY :]

        @pl.when(has_high)
        def _():
            ramps_low().wait_recv()
            around[16:24, :WX] = ramps_from_high[:, :WX]
            around[16:24, WX + RY :] = ramps_from_high[:, WX : WX + RY]

        @pl.when(has_left)
        def _():
            ramps_left().start()

        @pl.when(has_right)
        def _():
            ramps_right().start()

    def weights(rows):
        return lax.dot_general(
            rows[:, :WX].astype(jnp.bfloat16), rows[:, WX:].astype(jnp.bfloat16),
            (((0,), (0,)), ((), ())), preferred_element_type=jnp.float32,
        )

    def invert():
        inverse[...] = weights(around[...])[RX : RX + BX]

        @pl.when(has_left)
        def _():
            ramps_right().wait_recv()
            inverse[:RX] += weights(around_left[...])[RX + BX :]

        @pl.when(has_right)
        def _():
            ramps_left().wait_recv()
            inverse[RX:] += weights(around_right[...])[:RX]

        inverse[...] = 1.0 / jnp.maximum(inverse[...], 1.0)

    def step(slot, carry):
        @pl.when(slot < SLOTS)
        def _():
            z = slot

            @pl.when(z < NZ - 1)
            def _():
                along_y(z + 1)

            resample_x(z)
            start_y(slot)

        @pl.when(slot == LAG_Y + 1)
        def _():
            gather_ramps()

        ready = slot - LAG_Y

        @pl.when((ready >= 0) & (ready < SLOTS))
        def _():
            @pl.when(has_low)
            def _():
                to_high(ready).wait_recv()
                block[ready, :, :RY] += from_low[ready]

            @pl.when(has_high)
            def _():
                to_low(ready).wait_recv()
                block[ready, :, RY:] += from_high[ready]

            @pl.when(has_left)
            def _():
                to_left(ready).start()

            @pl.when(has_right)
            def _():
                to_right(ready).start()

        done = slot - LAG_X

        @pl.when((done >= 0) & (done < SLOTS))
        def _():
            @pl.when(has_left)
            def _():
                to_right(done).wait_recv()
                block[done, RX : 2 * RX] += from_left[done]

            @pl.when(has_right)
            def _():
                to_left(done).wait_recv()
                block[done, 2 * RX : 3 * RX] += from_right[done]

            @pl.when(done == 0)
            def _():
                invert()

            out[done] = block[done, RX : RX + BX] * inverse[...]

        return carry

    lax.fori_loop(1, SLOTS + LAG_X, step, 0)

    for present, copy in (
        (has_low, ramps_low), (has_high, ramps_high),
        (has_left, ramps_left), (has_right, ramps_right),
    ):
        @pl.when(present)
        def _(copy=copy):
            copy().wait_send()

    def finish(slot, carry):
        @pl.when(has_low)
        def _():
            to_low(slot).wait_send()

        @pl.when(has_high)
        def _():
            to_high(slot).wait_send()

        @pl.when(has_left)
        def _():
            to_left(slot).wait_send()

        @pl.when(has_right)
        def _():
            to_right(slot).wait_send()

        return carry

    lax.fori_loop(0, SLOTS, finish, 0)


def local(source_tiles, tile_offsets, tile_shifts, tile_counts):
    hbm = pl.BlockSpec(memory_space=pl.ANY)
    smem = pl.BlockSpec(memory_space=pltpu.SMEM)
    dma = pltpu.SemaphoreType.DMA
    return pl.pallas_call(
        kernel,
        out_shape=pltpu.VMEM((NZ, BX, BY), jnp.float32),
        in_specs=[hbm, smem, smem, smem],
        out_specs=pl.BlockSpec(memory_space=pltpu.VMEM),
        scratch_shapes=[
            pltpu.VMEM((CAP, NZ, TX, TY), jnp.bfloat16),
            pltpu.VMEM((SLOTS, WX, RY), jnp.float32),
            pltpu.VMEM((SLOTS, WX, RY), jnp.float32),
            pltpu.VMEM((SLOTS, WX, BY), jnp.float32),
            pltpu.VMEM((SLOTS, WX, RY), jnp.float32),
            pltpu.VMEM((SLOTS, WX, RY), jnp.float32),
            pltpu.VMEM((SLOTS, RX, BY), jnp.float32),
            pltpu.VMEM((SLOTS, RX, BY), jnp.float32),
            pltpu.VMEM((2, CAP, TX, WY), jnp.float32),
            pltpu.VMEM((CAP * 2 * TX, WY), jnp.bfloat16),
            pltpu.VMEM((CAP, TY, WY), jnp.bfloat16),
            pltpu.VMEM((WX, CAP * 2 * TX), jnp.bfloat16),
            pltpu.VMEM((BX, BY), jnp.float32),
            pltpu.VMEM((8, WX + WY), jnp.float32),
            pltpu.VMEM((8, WX + WY), jnp.float32),
            pltpu.VMEM((8, WX + WY), jnp.float32),
            pltpu.VMEM((24, WX + BY), jnp.float32),
            pltpu.VMEM((24, WX + BY), jnp.float32),
            pltpu.VMEM((24, WX + BY), jnp.float32),
            dma((NZ,)), dma((8,)),
            dma((SLOTS,)), dma((SLOTS,)), dma((SLOTS,)), dma((SLOTS,)),
            dma((SLOTS,)), dma((SLOTS,)), dma((SLOTS,)), dma((SLOTS,)),
        ],
        compiler_params=pltpu.CompilerParams(
            collective_id=0, has_side_effects=True, vmem_limit_bytes=54 * 1024 * 1024,
        ),
    )(source_tiles, tile_offsets, tile_shifts, tile_counts)


def solution(mesh):
    placed = (
        P(("gx", "gy"), None, None, None),
        P(None, ("gx", "gy")),
        P(("gx", "gy")),
        P(("gx", "gy")),
    )
    return jax.shard_map(
        local, mesh=mesh, in_specs=placed, out_specs=P(None, "gx", "gy"), check_vma=False
    )
```

```python
import jax
import jax.numpy as jnp
from jax import lax
from jax.experimental import pallas as pl
from jax.experimental.pallas import tpu as pltpu
from jax.sharding import PartitionSpec as P

NZ = 32
BX = 128
BY = 256
TX = 192
TY = 384
CAP = 3
RAMP = 32
RX = 64
RY = 128
WX = BX + 2 * RX
WY = BY + 2 * RY
AHEAD = 3
BEHIND = 12
HOLD = 6
GROUP = 2
EDGE = 4
LOT = 4
LOTS = (NZ - EDGE) // LOT
CENTRE = (NZ - 2 * EDGE) // 2
ROWS = 16
BLOCKS = WY // 128
MESH = pl.DeviceIdType.MESH


def ramp(places, length):
    return jnp.minimum(jnp.minimum(places + 1, length - places), RAMP)


def taps(places, length, fraction):
    inside = (places >= 0) & (places < length)
    blend = jnp.where(inside, ramp(places, length), 0).astype(jnp.float32)
    last = jnp.where(places == length - 1, fraction, 0.0)
    return blend, blend * (1.0 - fraction + last), blend * fraction


def kernel(
    tiles, offsets_hbm, shifts_hbm, counts_hbm, out,
    source, low_rim, high_rim, low_mid, high_mid,
    from_low_rim, from_high_rim, from_low_mid, from_high_mid,
    left, right, from_left, from_right,
    even, odd, placed, spread_y, spread_x, inverse,
    ramps, ramps_from_low, ramps_from_high, around, around_left, around_right,
    offsets, shifts, counts, number_sem, load_sem, ramp_sem, send_sem, recv_rim, recv_mid, recv_side,
):
    gx = lax.axis_index("gx")
    gy = lax.axis_index("gy")
    has_low, has_high = gy > 0, gy < lax.axis_size("gy") - 1
    has_left, has_right = gx > 0, gx < lax.axis_size("gx") - 1
    below, above = {"gy": gy - 1}, {"gy": gy + 1}
    before, after = {"gx": gx - 1}, {"gx": gx + 1}

    def load(i):
        z = NZ - 1 - i
        return pltpu.make_async_copy(tiles.at[:, z], source.at[:, z], load_sem.at[i])

    def load_lot(lot):
        span = pl.ds(NZ - EDGE - LOT * (lot + 1), LOT)
        return pltpu.make_async_copy(
            tiles.at[:, span], source.at[:, span], load_sem.at[EDGE + lot]
        )

    def remote(src, dst, send, recv, place):
        return pltpu.make_async_remote_copy(
            src_ref=src, dst_ref=dst, send_sem=send, recv_sem=recv,
            device_id=place, device_id_type=MESH,
        )

    def rim(way, z, count):
        src, dst, place = (
            (low_rim, from_high_rim, below), (high_rim, from_low_rim, above)
        )[way]
        span = pl.ds(z, count)
        return remote(
            src.at[span], dst.at[span], send_sem.at[way], recv_rim.at[way, z], place
        )

    def middle(way, z, count):
        src, dst, place = (
            (low_mid, from_high_mid, below), (high_mid, from_low_mid, above)
        )[way]
        span = pl.ds(z, count)
        return remote(
            src.at[span], dst.at[span], send_sem.at[2 + way], recv_mid.at[way, z // GROUP], place
        )

    def side(way, z, count):
        src, dst, place = ((left, from_right, before), (right, from_left, after))[way]
        span = pl.ds(z, count)
        inner = jnp.minimum(jnp.maximum(z - EDGE, 0) // 2, CENTRE)
        last = jnp.maximum(z - NZ + EDGE, 0)
        at = jnp.minimum(z, EDGE) + inner + last
        return remote(
            src.at[span], dst.at[span], send_sem.at[4 + way], recv_side.at[way, at], place
        )

    def ramp_y(way):
        dst, place = ((ramps_from_high, below), (ramps_from_low, above))[way]
        return remote(ramps, dst, ramp_sem.at[way], ramp_sem.at[2 + way], place)

    def ramp_x(way):
        dst, place = ((around_right, before), (around_left, after))[way]
        return remote(around, dst, ramp_sem.at[4 + way], ramp_sem.at[6 + way], place)

    y_ways = ((0, has_low, has_high), (1, has_high, has_low))
    x_ways = ((0, has_left, has_right), (1, has_right, has_left))

    def start(ways, make, *place):
        for way, sends, _ in ways:
            @pl.when(sends)
            def _(way=way):
                make(way, *place).start()

    def sent(ways, make, *place):
        for way, sends, _ in ways:
            @pl.when(sends)
            def _(way=way):
                make(way, *place).wait_send()

    def arrived(ways, make, *place):
        for way, _, receives in ways:
            @pl.when(receives)
            def _(way=way):
                make(way, *place).wait_recv()

    numbers = [
        pltpu.make_async_copy(src, dst, number_sem.at[n])
        for n, (src, dst) in enumerate(
            ((offsets_hbm, offsets), (shifts_hbm, shifts), (counts_hbm, counts))
        )
    ]
    for copy in numbers:
        copy.start()
    for i in range(3):
        load(i).start()

    barrier = pltpu.get_barrier_semaphore()
    neighbours = (
        (has_low, below), (has_high, above), (has_left, before), (has_right, after)
    )
    for present, place in neighbours:
        @pl.when(present)
        def _(place=place):
            pl.semaphore_signal(barrier, inc=1, device_id=place, device_id_type=MESH)

    for copy in numbers:
        copy.wait()
    starts_x, starts_y, parts, used, tops = [], [], [], [], []
    for k in range(CAP):
        code = shifts[k]
        starts_x.append(offsets[0, k] - gx * BX + RX)
        starts_y.append(offsets[1, k] - gy * BY + RY)
        tops.append(jnp.minimum(jnp.maximum(RX - starts_x[k], 0), RX))
        parts.append([
            ((code >> bits) & 3).astype(jnp.float32) * 0.25 for bits in (4, 2, 0)
        ])
        used.append(jnp.where(k < counts[0], 1.0, 0.0).astype(jnp.float32))

    taps_y = [
        taps(lax.broadcasted_iota(jnp.int32, (8, WY), 1) - starts_y[k], TY, parts[k][2])
        for k in range(CAP)
    ]
    for k in range(CAP):
        for r in range(0, TY, 64):
            apart = (
                lax.broadcasted_iota(jnp.int32, (64, WY), 0) + r
                - lax.broadcasted_iota(jnp.int32, (64, WY), 1) + starts_y[k]
            )
            own, following = taps_y[k][1][0:1], taps_y[k][2][0:1]
            spread_y[k, r : r + 64] = jnp.where(
                apart == 0, own, jnp.where(apart == 1, following, 0.0)
            ).astype(jnp.bfloat16)

    for k in range(CAP):
        place = lax.broadcasted_iota(jnp.int32, (WX, 128), 0) - starts_x[k]
        _, own, following = taps(place, TX, parts[k][1])
        spread_x[k, 0] = own * used[k]
        spread_x[k, 1] = following * used[k]
    placed[:, :, :RX] = jnp.zeros((CAP, BLOCKS, RX, 128), jnp.float32)
    placed[:, :, RX + TX :] = jnp.zeros((CAP, BLOCKS, RX + 8, 128), jnp.float32)

    ramps[...] = jnp.zeros_like(ramps)
    for k in range(CAP):
        blend = taps(
            lax.broadcasted_iota(jnp.int32, (8, WX), 1) - starts_x[k], TX, parts[k][1]
        )[0]
        ramps[k : k + 1, :WX] = blend[0:1] * used[k]
        ramps[k : k + 1, WX:] = taps_y[k][0][0:1]

    def along_y(z, *volumes):
        for k in range(CAP):
            rows = jnp.dot(
                source[k, z], spread_y[k], preferred_element_type=jnp.float32
            )
            for volume in volumes:
                volume[k] = rows

    load(0).wait()
    along_y(NZ - 1, even, odd)

    load(3).start()
    for lot in range(LOTS):
        load_lot(lot).start()

    pl.semaphore_wait(
        barrier, sum(present.astype(jnp.int32) for present, _ in neighbours)
    )

    def along_z(now, then):
        for k in range(CAP):
            depth_part = parts[k][0]
            for r in range(0, TX, ROWS):
                volume = (1.0 - depth_part) * now[k, r : r + ROWS] + (
                    depth_part * then[k, r : r + ROWS]
                )
                for n in range(BLOCKS):
                    placed[k, n, RX + r : RX + r + ROWS] = volume[:, n * 128 : (n + 1) * 128]

    def along_x(i, rims):
        for r in range(0, WX, ROWS):
            in_rim = r < RX or r >= RX + BX
            rim_row = r if r < RX else r - BX
            weights = [
                (spread_x[k, 0, r : r + ROWS], spread_x[k, 1, r : r + ROWS])
                for k in range(CAP)
            ]
            for n in range(BLOCKS):
                at_end = n in (0, BLOCKS - 1)
                if rims != (in_rim and at_end):
                    continue
                total = None
                for k in range(CAP):
                    first = tops[k] + r
                    term = weights[k][0] * placed[k, n, pl.ds(first, ROWS)] + (
                        weights[k][1] * placed[k, n, pl.ds(first + 1, ROWS)]
                    )
                    total = term if total is None else total + term
                if rims:
                    (low_rim if n == 0 else high_rim)[i, rim_row : rim_row + ROWS] = total
                elif at_end:
                    (low_mid if n == 0 else high_mid)[i, r - RX : r - RX + ROWS] = total
                else:
                    lanes = slice((n - 1) * 128, n * 128)
                    if r < RX:
                        left[i, r : r + ROWS, lanes] = total
                    elif in_rim:
                        right[i, r - RX - BX : r - RX - BX + ROWS, lanes] = total
                    else:
                        out[NZ - 1 - i, r - RX : r - RX + ROWS, lanes] = total

    def gather_ramps():
        around[...] = jnp.zeros_like(around)
        around[0:8, :WX] = ramps[:, :WX]
        around[0:8, WX:] = ramps[:, WX + RY : WX + RY + BY]
        arrived(y_ways, ramp_y)

        @pl.when(has_low)
        def _():
            around[8:16, :WX] = ramps_from_low[:, :WX]
            around[8:16, WX : WX + RY] = ramps_from_low[:, WX + RY + BY :]

        @pl.when(has_high)
        def _():
            around[16:24, :WX] = ramps_from_high[:, :WX]
            around[16:24, WX + RY :] = ramps_from_high[:, WX : WX + RY]

        start(x_ways, ramp_x)

    def weights_of(rows):
        return lax.dot_general(
            rows[:, :WX].astype(jnp.bfloat16), rows[:, WX:].astype(jnp.bfloat16),
            (((0,), (0,)), ((), ())), preferred_element_type=jnp.float32,
        )

    def invert():
        inverse[...] = weights_of(around[...])[RX : RX + BX]
        arrived(x_ways, ramp_x)

        @pl.when(has_left)
        def _():
            inverse[:RX] += weights_of(around_left[...])[RX + BX :]

        @pl.when(has_right)
        def _():
            inverse[RX:] += weights_of(around_right[...])[:RX]

        inverse[...] = 1.0 / jnp.maximum(inverse[...], 1.0)

    def sides(z):
        @pl.when(has_low)
        def _():
            left[z, :, :RY] += from_low_rim[z, :RX]
            right[z, :, :RY] += from_low_rim[z, RX:]

        @pl.when(has_high)
        def _():
            left[z, :, RY:] += from_high_rim[z, :RX]
            right[z, :, RY:] += from_high_rim[z, RX:]

    def finish(i):
        z = NZ - 1 - i

        @pl.when(has_low)
        def _():
            out[z, :, :RY] += from_low_mid[i]

        @pl.when(has_high)
        def _():
            out[z, :, RY:] += from_high_mid[i]

        @pl.when(has_left)
        def _():
            out[z, :RX] += from_left[i]

        @pl.when(has_right)
        def _():
            out[z, RX:] += from_right[i]

        out[z] *= inverse[...]

    def alone(i):
        return (i < EDGE) | (i >= NZ - EDGE)

    def step(i, now, then):
        @pl.when(i < NZ)
        def _():
            z = NZ - 2 - i

            @pl.when(i + 1 < EDGE)
            def _():
                load(i + 1).wait()

            @pl.when((i + 1 >= EDGE) & (i + 1 < NZ) & ((i + 1) % LOT == 0))
            def _():
                load_lot((i + 1 - EDGE) // LOT).wait()

            along_z(now, then)
            along_y(jnp.maximum(z, 0), then)
            along_x(i, True)
            along_x(i, False)
            start(y_ways, rim, i, 1)

            @pl.when(i == 0)
            def _():
                start(y_ways, ramp_y)

            @pl.when((i % GROUP == GROUP - 1) & (i > HOLD))
            def _():
                start(y_ways, middle, i - HOLD - GROUP + 1, GROUP)

            @pl.when(i == NZ - 1)
            def _():
                for k in range(HOLD, 0, -GROUP):
                    start(y_ways, middle, NZ - k, GROUP)

        ready = i - AHEAD

        @pl.when((ready >= 0) & (ready < NZ))
        def _():
            arrived(y_ways, rim, ready, 1)
            sides(ready)

            @pl.when(alone(ready))
            def _():
                start(x_ways, side, ready, 1)

            @pl.when(jnp.logical_not(alone(ready)) & (ready % 2 == 1))
            def _():
                start(x_ways, side, ready - 1, 2)

            @pl.when(ready == 3)
            def _():
                gather_ramps()

        done = i - BEHIND

        @pl.when((done >= 0) & (done < NZ))
        def _():
            @pl.when(done == 0)
            def _():
                invert()

            @pl.when(done % GROUP == 0)
            def _():
                arrived(y_ways, middle, done, GROUP)

            @pl.when(alone(done))
            def _():
                arrived(x_ways, side, done, 1)

            @pl.when(jnp.logical_not(alone(done)) & (done % 2 == 0))
            def _():
                arrived(x_ways, side, done, 2)

            finish(done)

    def two_steps(pair, carry):
        step(2 * pair, even, odd)
        step(2 * pair + 1, odd, even)
        return carry

    lax.fori_loop(0, (NZ + BEHIND) // 2, two_steps, 0)

    sent(y_ways, ramp_y)
    sent(x_ways, ramp_x)

    sent(y_ways, rim, 0, NZ)
    sent(y_ways, middle, 0, NZ)
    sent(x_ways, side, 0, NZ)


def local(source_tiles, tile_offsets, tile_shifts, tile_counts):
    hbm = pl.BlockSpec(memory_space=pl.ANY)
    dma = pltpu.SemaphoreType.DMA
    volume = pltpu.VMEM((CAP, TX, WY), jnp.float32)
    halo = pltpu.VMEM((NZ, BX, RY), jnp.float32)
    flank = pltpu.VMEM((NZ, RX, BY), jnp.float32)
    ramps = pltpu.VMEM((8, WX + WY), jnp.float32)
    around = pltpu.VMEM((24, WX + BY), jnp.float32)
    return pl.pallas_call(
        kernel,
        out_shape=pltpu.VMEM((NZ, BX, BY), jnp.float32),
        in_specs=[hbm, hbm, hbm, hbm],
        out_specs=pl.BlockSpec(memory_space=pltpu.VMEM),
        scratch_shapes=[
            pltpu.VMEM((CAP, NZ, TX, TY), jnp.bfloat16),
            halo, halo, halo, halo, halo, halo, halo, halo,
            flank, flank, flank, flank,
            volume, volume,
            pltpu.VMEM((CAP, BLOCKS, RX + TX + RX + 8, 128), jnp.float32),
            pltpu.VMEM((CAP, TY, WY), jnp.bfloat16),
            pltpu.VMEM((CAP, 2, WX, 128), jnp.float32),
            pltpu.VMEM((BX, BY), jnp.float32),
            ramps, ramps, ramps, around, around, around,
            pltpu.SMEM((2, CAP), jnp.int32),
            pltpu.SMEM((CAP,), jnp.int32),
            pltpu.SMEM((1,), jnp.int32),
            dma((3,)), dma((EDGE + LOTS,)), dma((8,)),
            dma((6,)), dma((2, NZ)), dma((2, NZ // GROUP)), dma((2, 2 * EDGE + CENTRE)),
        ],
        compiler_params=pltpu.CompilerParams(
            collective_id=0, has_side_effects=True, vmem_limit_bytes=54 * 1024 * 1024,
        ),
    )(source_tiles, tile_offsets, tile_shifts, tile_counts)


def solution(mesh):
    placed = (
        P(("gx", "gy"), None, None, None),
        P(None, ("gx", "gy")),
        P(("gx", "gy")),
        P(("gx", "gy")),
    )
    return jax.shard_map(
        local, mesh=mesh, in_specs=placed, out_specs=P(None, "gx", "gy"), check_vma=False
    )
```

```python
import jax
import jax.numpy as jnp
from jax import lax
from jax.experimental import pallas as pl
from jax.experimental.pallas import tpu as pltpu
from jax.sharding import PartitionSpec as P

NZ = 32
BX = 128
BY = 256
TX = 192
TY = 384
CAP = 3
RAMP = 32
RX = 64
RY = 128
WX = BX + 2 * RX
WY = BY + 2 * RY
AHEAD = 3
BEHIND = 12
HOLD = 6
GROUP = 2
EDGE = 4
LOT = 4
LOTS = (NZ - EDGE) // LOT
CENTRE = (NZ - 2 * EDGE) // 2
ROWS = 16
BLOCKS = WY // 128
MESH = pl.DeviceIdType.MESH


def ramp(places, length):
    return jnp.minimum(jnp.minimum(places + 1, length - places), RAMP)


def taps(places, length, fraction):
    inside = (places >= 0) & (places < length)
    blend = jnp.where(inside, ramp(places, length), 0).astype(jnp.float32)
    last = jnp.where(places == length - 1, fraction, 0.0)
    return blend, blend * (1.0 - fraction + last), blend * fraction


def kernel(
    tiles, offsets_hbm, shifts_hbm, counts_hbm, out,
    source, low_rim, high_rim, low_mid, high_mid,
    from_low_rim, from_high_rim, from_low_mid, from_high_mid,
    left, right, from_left, from_right,
    even, odd, placed, spread_y, spread_x, inverse,
    ramps, ramps_from_low, ramps_from_high, around, around_left, around_right,
    offsets, shifts, counts, number_sem, load_sem, ramp_sem, send_sem, recv_rim, recv_mid, recv_side,
):
    gx = lax.axis_index("gx")
    gy = lax.axis_index("gy")
    has_low, has_high = gy > 0, gy < lax.axis_size("gy") - 1
    has_left, has_right = gx > 0, gx < lax.axis_size("gx") - 1
    below, above = {"gy": gy - 1}, {"gy": gy + 1}
    before, after = {"gx": gx - 1}, {"gx": gx + 1}

    def load(i):
        z = NZ - 1 - i
        return pltpu.make_async_copy(tiles.at[:, z], source.at[:, z], load_sem.at[i])

    def load_lot(lot):
        span = pl.ds(NZ - EDGE - LOT * (lot + 1), LOT)
        return pltpu.make_async_copy(
            tiles.at[:, span], source.at[:, span], load_sem.at[EDGE + lot]
        )

    def remote(src, dst, send, recv, place):
        return pltpu.make_async_remote_copy(
            src_ref=src, dst_ref=dst, send_sem=send, recv_sem=recv,
            device_id=place, device_id_type=MESH,
        )

    def rim(way, z, count):
        src, dst, place = (
            (low_rim, from_high_rim, below), (high_rim, from_low_rim, above)
        )[way]
        span = pl.ds(z, count)
        return remote(
            src.at[span], dst.at[span], send_sem.at[way], recv_rim.at[way, z % (2 * AHEAD + 2)], place
        )

    def middle(way, z, count):
        src, dst, place = (
            (low_mid, from_high_mid, below), (high_mid, from_low_mid, above)
        )[way]
        span = pl.ds(z, count)
        return remote(
            src.at[span], dst.at[span], send_sem.at[2 + way], recv_mid.at[way, z // GROUP], place
        )

    def side(way, z, count):
        src, dst, place = ((left, from_right, before), (right, from_left, after))[way]
        span = pl.ds(z, count)
        inner = jnp.minimum(jnp.maximum(z - EDGE, 0) // 2, CENTRE)
        last = jnp.maximum(z - NZ + EDGE, 0)
        at = jnp.minimum(z, EDGE) + inner + last
        return remote(
            src.at[span], dst.at[span], send_sem.at[4 + way], recv_side.at[way, at], place
        )

    def ramp_y(way):
        dst, place = ((ramps_from_high, below), (ramps_from_low, above))[way]
        return remote(ramps, dst, ramp_sem.at[way], ramp_sem.at[2 + way], place)

    def ramp_x(way):
        dst, place = ((around_right, before), (around_left, after))[way]
        return remote(around, dst, ramp_sem.at[4 + way], ramp_sem.at[6 + way], place)

    y_ways = ((0, has_low, has_high), (1, has_high, has_low))
    x_ways = ((0, has_left, has_right), (1, has_right, has_left))

    def start(ways, make, *place):
        for way, sends, _ in ways:
            @pl.when(sends)
            def _(way=way):
                make(way, *place).start()

    def sent(ways, make, *place):
        for way, sends, _ in ways:
            @pl.when(sends)
            def _(way=way):
                make(way, *place).wait_send()

    def arrived(ways, make, *place):
        for way, _, receives in ways:
            @pl.when(receives)
            def _(way=way):
                make(way, *place).wait_recv()

    numbers = [
        pltpu.make_async_copy(src, dst, number_sem.at[n])
        for n, (src, dst) in enumerate(
            ((offsets_hbm, offsets), (shifts_hbm, shifts), (counts_hbm, counts))
        )
    ]
    for copy in numbers:
        copy.start()
    for i in range(3):
        load(i).start()

    barrier = pltpu.get_barrier_semaphore()
    neighbours = (
        (has_low, below), (has_high, above), (has_left, before), (has_right, after)
    )
    for present, place in neighbours:
        @pl.when(present)
        def _(place=place):
            pl.semaphore_signal(barrier, inc=1, device_id=place, device_id_type=MESH)

    for copy in numbers:
        copy.wait()
    starts_x, starts_y, parts, used, tops = [], [], [], [], []
    for k in range(CAP):
        code = shifts[k]
        starts_x.append(offsets[0, k] - gx * BX + RX)
        starts_y.append(offsets[1, k] - gy * BY + RY)
        tops.append(jnp.minimum(jnp.maximum(RX - starts_x[k], 0), RX))
        parts.append([
            ((code >> bits) & 3).astype(jnp.float32) * 0.25 for bits in (4, 2, 0)
        ])
        used.append(jnp.where(k < counts[0], 1.0, 0.0).astype(jnp.float32))

    taps_y = [
        taps(lax.broadcasted_iota(jnp.int32, (8, WY), 1) - starts_y[k], TY, parts[k][2])
        for k in range(CAP)
    ]
    for k in range(CAP):
        for r in range(0, TY, 64):
            apart = (
                lax.broadcasted_iota(jnp.int32, (64, WY), 0) + r
                - lax.broadcasted_iota(jnp.int32, (64, WY), 1) + starts_y[k]
            )
            own, following = taps_y[k][1][0:1], taps_y[k][2][0:1]
            spread_y[k, r : r + 64] = jnp.where(
                apart == 0, own, jnp.where(apart == 1, following, 0.0)
            ).astype(jnp.bfloat16)

    for k in range(CAP):
        place = lax.broadcasted_iota(jnp.int32, (WX, 128), 0) - starts_x[k]
        _, own, following = taps(place, TX, parts[k][1])
        spread_x[k, 0] = own * used[k]
        spread_x[k, 1] = following * used[k]
    placed[:, :, :RX] = jnp.zeros((CAP, BLOCKS, RX, 128), jnp.float32)
    placed[:, :, RX + TX :] = jnp.zeros((CAP, BLOCKS, RX + 8, 128), jnp.float32)

    ramps[...] = jnp.zeros_like(ramps)
    for k in range(CAP):
        blend = taps(
            lax.broadcasted_iota(jnp.int32, (8, WX), 1) - starts_x[k], TX, parts[k][1]
        )[0]
        ramps[k : k + 1, :WX] = blend[0:1] * used[k]
        ramps[k : k + 1, WX:] = taps_y[k][0][0:1]

    def along_y(z, *volumes):
        for k in range(CAP):
            rows = jnp.dot(
                source[k, z], spread_y[k], preferred_element_type=jnp.float32
            )
            for volume in volumes:
                volume[k] = rows

    load(0).wait()
    along_y(NZ - 1, even, odd)

    load(3).start()
    for lot in range(LOTS):
        load_lot(lot).start()

    pl.semaphore_wait(
        barrier, sum(present.astype(jnp.int32) for present, _ in neighbours)
    )

    def along_z(now, then):
        for k in range(CAP):
            depth_part = parts[k][0]
            for r in range(0, TX, ROWS):
                volume = (1.0 - depth_part) * now[k, r : r + ROWS] + (
                    depth_part * then[k, r : r + ROWS]
                )
                for n in range(BLOCKS):
                    placed[k, n, RX + r : RX + r + ROWS] = volume[:, n * 128 : (n + 1) * 128]

    def along_x(i, rims):
        for r in range(0, WX, ROWS):
            in_rim = r < RX or r >= RX + BX
            rim_row = r if r < RX else r - BX
            weights = [
                (spread_x[k, 0, r : r + ROWS], spread_x[k, 1, r : r + ROWS])
                for k in range(CAP)
            ]
            for n in range(BLOCKS):
                at_end = n in (0, BLOCKS - 1)
                if rims != (in_rim and at_end):
                    continue
                total = None
                for k in range(CAP):
                    first = tops[k] + r
                    term = weights[k][0] * placed[k, n, pl.ds(first, ROWS)] + (
                        weights[k][1] * placed[k, n, pl.ds(first + 1, ROWS)]
                    )
                    total = term if total is None else total + term
                if rims:
                    (low_rim if n == 0 else high_rim)[i, rim_row : rim_row + ROWS] = total
                elif at_end:
                    (low_mid if n == 0 else high_mid)[i, r - RX : r - RX + ROWS] = total
                else:
                    lanes = slice((n - 1) * 128, n * 128)
                    if r < RX:
                        left[i, r : r + ROWS, lanes] = total
                    elif in_rim:
                        right[i, r - RX - BX : r - RX - BX + ROWS, lanes] = total
                    else:
                        out[NZ - 1 - i, r - RX : r - RX + ROWS, lanes] = total

    def gather_ramps():
        around[...] = jnp.zeros_like(around)
        around[0:8, :WX] = ramps[:, :WX]
        around[0:8, WX:] = ramps[:, WX + RY : WX + RY + BY]
        arrived(y_ways, ramp_y)

        @pl.when(has_low)
        def _():
            around[8:16, :WX] = ramps_from_low[:, :WX]
            around[8:16, WX : WX + RY] = ramps_from_low[:, WX + RY + BY :]

        @pl.when(has_high)
        def _():
            around[16:24, :WX] = ramps_from_high[:, :WX]
            around[16:24, WX + RY :] = ramps_from_high[:, WX : WX + RY]

        start(x_ways, ramp_x)

    def weights_of(rows):
        return lax.dot_general(
            rows[:, :WX].astype(jnp.bfloat16), rows[:, WX:].astype(jnp.bfloat16),
            (((0,), (0,)), ((), ())), preferred_element_type=jnp.float32,
        )

    def invert():
        inverse[...] = weights_of(around[...])[RX : RX + BX]
        arrived(x_ways, ramp_x)

        @pl.when(has_left)
        def _():
            inverse[:RX] += weights_of(around_left[...])[RX + BX :]

        @pl.when(has_right)
        def _():
            inverse[RX:] += weights_of(around_right[...])[:RX]

        inverse[...] = 1.0 / jnp.maximum(inverse[...], 1.0)

    def sides(z):
        @pl.when(has_low)
        def _():
            left[z, :, :RY] += from_low_rim[z, :RX]
            right[z, :, :RY] += from_low_rim[z, RX:]

        @pl.when(has_high)
        def _():
            left[z, :, RY:] += from_high_rim[z, :RX]
            right[z, :, RY:] += from_high_rim[z, RX:]

    def finish(i):
        z = NZ - 1 - i

        @pl.when(has_low)
        def _():
            out[z, :, :RY] += from_low_mid[i]

        @pl.when(has_high)
        def _():
            out[z, :, RY:] += from_high_mid[i]

        @pl.when(has_left)
        def _():
            out[z, :RX] += from_left[i]

        @pl.when(has_right)
        def _():
            out[z, RX:] += from_right[i]

        out[z] *= inverse[...]

    def alone(i):
        return (i < EDGE) | (i >= NZ - EDGE)

    def step(i, now, then):
        @pl.when(i < NZ)
        def _():
            z = NZ - 2 - i

            @pl.when(i + 1 < EDGE)
            def _():
                load(i + 1).wait()

            @pl.when((i + 1 >= EDGE) & (i + 1 < NZ) & ((i + 1) % LOT == 0))
            def _():
                load_lot((i + 1 - EDGE) // LOT).wait()

            along_z(now, then)
            along_y(jnp.maximum(z, 0), then)
            along_x(i, True)
            along_x(i, False)
            start(y_ways, rim, i, 1)

            @pl.when(i == 0)
            def _():
                start(y_ways, ramp_y)

            @pl.when((i % GROUP == GROUP - 1) & (i > HOLD))
            def _():
                start(y_ways, middle, i - HOLD - GROUP + 1, GROUP)

            @pl.when(i == NZ - 1)
            def _():
                for k in range(HOLD, 0, -GROUP):
                    start(y_ways, middle, NZ - k, GROUP)

        ready = i - AHEAD

        @pl.when((ready >= 0) & (ready < NZ))
        def _():
            arrived(y_ways, rim, ready, 1)
            sides(ready)

            @pl.when(alone(ready))
            def _():
                start(x_ways, side, ready, 1)

            @pl.when(jnp.logical_not(alone(ready)) & (ready % 2 == 1))
            def _():
                start(x_ways, side, ready - 1, 2)

            @pl.when(ready == 3)
            def _():
                gather_ramps()

        done = i - BEHIND

        @pl.when((done >= 0) & (done < NZ))
        def _():
            @pl.when(done == 0)
            def _():
                invert()

            @pl.when(done % GROUP == 0)
            def _():
                arrived(y_ways, middle, done, GROUP)

            @pl.when(alone(done))
            def _():
                arrived(x_ways, side, done, 1)

            @pl.when(jnp.logical_not(alone(done)) & (done % 2 == 0))
            def _():
                arrived(x_ways, side, done, 2)

            finish(done)

    def two_steps(pair, carry):
        step(2 * pair, even, odd)
        step(2 * pair + 1, odd, even)
        return carry

    lax.fori_loop(0, (NZ + BEHIND) // 2, two_steps, 0)

    sent(y_ways, ramp_y)
    sent(x_ways, ramp_x)

    sent(y_ways, rim, 0, NZ)
    sent(y_ways, middle, 0, NZ)
    sent(x_ways, side, 0, NZ)


def local(source_tiles, tile_offsets, tile_shifts, tile_counts):
    hbm = pl.BlockSpec(memory_space=pl.ANY)
    dma = pltpu.SemaphoreType.DMA
    volume = pltpu.VMEM((CAP, TX, WY), jnp.float32)
    halo = pltpu.VMEM((NZ, BX, RY), jnp.float32)
    flank = pltpu.VMEM((NZ, RX, BY), jnp.float32)
    ramps = pltpu.VMEM((8, WX + WY), jnp.float32)
    around = pltpu.VMEM((24, WX + BY), jnp.float32)
    return pl.pallas_call(
        kernel,
        out_shape=pltpu.VMEM((NZ, BX, BY), jnp.float32),
        in_specs=[hbm, hbm, hbm, hbm],
        out_specs=pl.BlockSpec(memory_space=pltpu.VMEM),
        scratch_shapes=[
            pltpu.VMEM((CAP, NZ, TX, TY), jnp.bfloat16),
            halo, halo, halo, halo, halo, halo, halo, halo,
            flank, flank, flank, flank,
            volume, volume,
            pltpu.VMEM((CAP, BLOCKS, RX + TX + RX + 8, 128), jnp.float32),
            pltpu.VMEM((CAP, TY, WY), jnp.bfloat16),
            pltpu.VMEM((CAP, 2, WX, 128), jnp.float32),
            pltpu.VMEM((BX, BY), jnp.float32),
            ramps, ramps, ramps, around, around, around,
            pltpu.SMEM((2, CAP), jnp.int32),
            pltpu.SMEM((CAP,), jnp.int32),
            pltpu.SMEM((1,), jnp.int32),
            dma((3,)), dma((EDGE + LOTS,)), dma((8,)),
            dma((6,)), dma((2, 2 * AHEAD + 2)), dma((2, NZ // GROUP)), dma((2, 2 * EDGE + CENTRE)),
        ],
        compiler_params=pltpu.CompilerParams(
            collective_id=0, has_side_effects=True, vmem_limit_bytes=54 * 1024 * 1024,
        ),
    )(source_tiles, tile_offsets, tile_shifts, tile_counts)


def solution(mesh):
    placed = (
        P(("gx", "gy"), None, None, None),
        P(None, ("gx", "gy")),
        P(("gx", "gy")),
        P(("gx", "gy")),
    )
    return jax.shard_map(
        local, mesh=mesh, in_specs=placed, out_specs=P(None, "gx", "gy"), check_vma=False
    )
```

```python
import jax
import jax.numpy as jnp
from jax import lax
from jax.experimental import pallas as pl
from jax.experimental.pallas import tpu as pltpu
from jax.sharding import PartitionSpec as P

NZ = 32
BX = 128
BY = 256
TX = 192
TY = 384
CAP = 3
RAMP = 32
RX = 64
RY = 128
WX = BX + 2 * RX
WY = BY + 2 * RY
AHEAD = 3
BEHIND = 14
HOLD = 4
GROUP = 4
EDGE = 4
LOT = 4
LOTS = (NZ - EDGE) // LOT
CENTRE = (NZ - 2 * EDGE) // 2
ROWS = 16
BLOCKS = WY // 128
MESH = pl.DeviceIdType.MESH


def ramp(places, length):
    return jnp.minimum(jnp.minimum(places + 1, length - places), RAMP)


def taps(places, length, fraction):
    inside = (places >= 0) & (places < length)
    blend = jnp.where(inside, ramp(places, length), 0).astype(jnp.float32)
    last = jnp.where(places == length - 1, fraction, 0.0)
    return blend, blend * (1.0 - fraction + last), blend * fraction


def kernel(
    tiles, offsets_hbm, shifts_hbm, counts_hbm, out,
    source, low_rim, high_rim, low_mid, high_mid,
    from_low_rim, from_high_rim, from_low_mid, from_high_mid,
    left, right, from_left, from_right,
    even, odd, placed, spread_y, spread_x, inverse,
    ramps, ramps_from_low, ramps_from_high, around, around_left, around_right,
    offsets, shifts, counts, number_sem, load_sem, ramp_sem, send_sem, recv_rim, recv_mid, recv_side,
):
    gx = lax.axis_index("gx")
    gy = lax.axis_index("gy")
    has_low, has_high = gy > 0, gy < lax.axis_size("gy") - 1
    has_left, has_right = gx > 0, gx < lax.axis_size("gx") - 1
    below, above = {"gy": gy - 1}, {"gy": gy + 1}
    before, after = {"gx": gx - 1}, {"gx": gx + 1}

    def load(i):
        z = NZ - 1 - i
        return pltpu.make_async_copy(tiles.at[:, z], source.at[:, z], load_sem.at[i])

    def load_lot(lot):
        span = pl.ds(NZ - EDGE - LOT * (lot + 1), LOT)
        return pltpu.make_async_copy(
            tiles.at[:, span], source.at[:, span], load_sem.at[EDGE + lot]
        )

    def remote(src, dst, send, recv, place):
        return pltpu.make_async_remote_copy(
            src_ref=src, dst_ref=dst, send_sem=send, recv_sem=recv,
            device_id=place, device_id_type=MESH,
        )

    def rim(way, z, count):
        src, dst, place = (
            (low_rim, from_high_rim, below), (high_rim, from_low_rim, above)
        )[way]
        span = pl.ds(z, count)
        return remote(
            src.at[span], dst.at[span], send_sem.at[way], recv_rim.at[way, z % (2 * AHEAD + 2)], place
        )

    def middle(way, z, count):
        src, dst, place = (
            (low_mid, from_high_mid, below), (high_mid, from_low_mid, above)
        )[way]
        span = pl.ds(z, count)
        return remote(
            src.at[span], dst.at[span], send_sem.at[2 + way], recv_mid.at[way, z // GROUP], place
        )

    def side(way, z, count):
        src, dst, place = ((left, from_right, before), (right, from_left, after))[way]
        span = pl.ds(z, count)
        inner = jnp.minimum(jnp.maximum(z - EDGE, 0) // 2, CENTRE)
        last = jnp.maximum(z - NZ + EDGE, 0)
        at = jnp.minimum(z, EDGE) + inner + last
        return remote(
            src.at[span], dst.at[span], send_sem.at[4 + way], recv_side.at[way, at], place
        )

    def ramp_y(way):
        dst, place = ((ramps_from_high, below), (ramps_from_low, above))[way]
        return remote(ramps, dst, ramp_sem.at[way], ramp_sem.at[2 + way], place)

    def ramp_x(way):
        dst, place = ((around_right, before), (around_left, after))[way]
        return remote(around, dst, ramp_sem.at[4 + way], ramp_sem.at[6 + way], place)

    y_ways = ((0, has_low, has_high), (1, has_high, has_low))
    x_ways = ((0, has_left, has_right), (1, has_right, has_left))

    def start(ways, make, *place):
        for way, sends, _ in ways:
            @pl.when(sends)
            def _(way=way):
                make(way, *place).start()

    def sent(ways, make, *place):
        for way, sends, _ in ways:
            @pl.when(sends)
            def _(way=way):
                make(way, *place).wait_send()

    def arrived(ways, make, *place):
        for way, _, receives in ways:
            @pl.when(receives)
            def _(way=way):
                make(way, *place).wait_recv()

    numbers = [
        pltpu.make_async_copy(src, dst, number_sem.at[n])
        for n, (src, dst) in enumerate(
            ((offsets_hbm, offsets), (shifts_hbm, shifts), (counts_hbm, counts))
        )
    ]
    for copy in numbers:
        copy.start()
    for i in range(3):
        load(i).start()

    barrier = pltpu.get_barrier_semaphore()
    neighbours = (
        (has_low, below), (has_high, above), (has_left, before), (has_right, after)
    )
    for present, place in neighbours:
        @pl.when(present)
        def _(place=place):
            pl.semaphore_signal(barrier, inc=1, device_id=place, device_id_type=MESH)

    for copy in numbers:
        copy.wait()
    starts_x, starts_y, parts, used, tops = [], [], [], [], []
    for k in range(CAP):
        code = shifts[k]
        starts_x.append(offsets[0, k] - gx * BX + RX)
        starts_y.append(offsets[1, k] - gy * BY + RY)
        tops.append(jnp.minimum(jnp.maximum(RX - starts_x[k], 0), RX))
        parts.append([
            ((code >> bits) & 3).astype(jnp.float32) * 0.25 for bits in (4, 2, 0)
        ])
        used.append(jnp.where(k < counts[0], 1.0, 0.0).astype(jnp.float32))

    taps_y = [
        taps(lax.broadcasted_iota(jnp.int32, (8, WY), 1) - starts_y[k], TY, parts[k][2])
        for k in range(CAP)
    ]
    for k in range(CAP):
        for r in range(0, TY, 64):
            apart = (
                lax.broadcasted_iota(jnp.int32, (64, WY), 0) + r
                - lax.broadcasted_iota(jnp.int32, (64, WY), 1) + starts_y[k]
            )
            own, following = taps_y[k][1][0:1], taps_y[k][2][0:1]
            spread_y[k, r : r + 64] = jnp.where(
                apart == 0, own, jnp.where(apart == 1, following, 0.0)
            ).astype(jnp.bfloat16)

    for k in range(CAP):
        place = lax.broadcasted_iota(jnp.int32, (WX, 128), 0) - starts_x[k]
        _, own, following = taps(place, TX, parts[k][1])
        spread_x[k, 0] = own * used[k]
        spread_x[k, 1] = following * used[k]
    placed[:, :, :RX] = jnp.zeros((CAP, BLOCKS, RX, 128), jnp.float32)
    placed[:, :, RX + TX :] = jnp.zeros((CAP, BLOCKS, RX + 8, 128), jnp.float32)

    ramps[...] = jnp.zeros_like(ramps)
    for k in range(CAP):
        blend = taps(
            lax.broadcasted_iota(jnp.int32, (8, WX), 1) - starts_x[k], TX, parts[k][1]
        )[0]
        ramps[k : k + 1, :WX] = blend[0:1] * used[k]
        ramps[k : k + 1, WX:] = taps_y[k][0][0:1]

    def along_y(z, *volumes):
        for k in range(CAP):
            rows = jnp.dot(
                source[k, z], spread_y[k], preferred_element_type=jnp.float32
            )
            for volume in volumes:
                volume[k] = rows

    load(0).wait()
    along_y(NZ - 1, even, odd)

    load(3).start()
    for lot in range(LOTS):
        load_lot(lot).start()

    pl.semaphore_wait(
        barrier, sum(present.astype(jnp.int32) for present, _ in neighbours)
    )

    def along_z(now, then):
        for k in range(CAP):
            depth_part = parts[k][0]
            for r in range(0, TX, ROWS):
                volume = (1.0 - depth_part) * now[k, r : r + ROWS] + (
                    depth_part * then[k, r : r + ROWS]
                )
                for n in range(BLOCKS):
                    placed[k, n, RX + r : RX + r + ROWS] = volume[:, n * 128 : (n + 1) * 128]

    def along_x(i, rims):
        for r in range(0, WX, ROWS):
            in_rim = r < RX or r >= RX + BX
            rim_row = r if r < RX else r - BX
            weights = [
                (spread_x[k, 0, r : r + ROWS], spread_x[k, 1, r : r + ROWS])
                for k in range(CAP)
            ]
            for n in range(BLOCKS):
                at_end = n in (0, BLOCKS - 1)
                if rims != (in_rim and at_end):
                    continue
                total = None
                for k in range(CAP):
                    first = tops[k] + r
                    term = weights[k][0] * placed[k, n, pl.ds(first, ROWS)] + (
                        weights[k][1] * placed[k, n, pl.ds(first + 1, ROWS)]
                    )
                    total = term if total is None else total + term
                if rims:
                    (low_rim if n == 0 else high_rim)[i, rim_row : rim_row + ROWS] = total
                elif at_end:
                    (low_mid if n == 0 else high_mid)[i, r - RX : r - RX + ROWS] = total
                else:
                    lanes = slice((n - 1) * 128, n * 128)
                    if r < RX:
                        left[i, r : r + ROWS, lanes] = total
                    elif in_rim:
                        right[i, r - RX - BX : r - RX - BX + ROWS, lanes] = total
                    else:
                        out[NZ - 1 - i, r - RX : r - RX + ROWS, lanes] = total

    def gather_ramps():
        around[...] = jnp.zeros_like(around)
        around[0:8, :WX] = ramps[:, :WX]
        around[0:8, WX:] = ramps[:, WX + RY : WX + RY + BY]
        arrived(y_ways, ramp_y)

        @pl.when(has_low)
        def _():
            around[8:16, :WX] = ramps_from_low[:, :WX]
            around[8:16, WX : WX + RY] = ramps_from_low[:, WX + RY + BY :]

        @pl.when(has_high)
        def _():
            around[16:24, :WX] = ramps_from_high[:, :WX]
            around[16:24, WX + RY :] = ramps_from_high[:, WX : WX + RY]

        start(x_ways, ramp_x)

    def weights_of(rows):
        return lax.dot_general(
            rows[:, :WX].astype(jnp.bfloat16), rows[:, WX:].astype(jnp.bfloat16),
            (((0,), (0,)), ((), ())), preferred_element_type=jnp.float32,
        )

    def invert():
        inverse[...] = weights_of(around[...])[RX : RX + BX]
        arrived(x_ways, ramp_x)

        @pl.when(has_left)
        def _():
            inverse[:RX] += weights_of(around_left[...])[RX + BX :]

        @pl.when(has_right)
        def _():
            inverse[RX:] += weights_of(around_right[...])[:RX]

        inverse[...] = 1.0 / jnp.maximum(inverse[...], 1.0)

    def sides(z):
        @pl.when(has_low)
        def _():
            left[z, :, :RY] += from_low_rim[z, :RX]
            right[z, :, :RY] += from_low_rim[z, RX:]

        @pl.when(has_high)
        def _():
            left[z, :, RY:] += from_high_rim[z, :RX]
            right[z, :, RY:] += from_high_rim[z, RX:]

    def finish(i):
        z = NZ - 1 - i

        @pl.when(has_low)
        def _():
            out[z, :, :RY] += from_low_mid[i]

        @pl.when(has_high)
        def _():
            out[z, :, RY:] += from_high_mid[i]

        @pl.when(has_left)
        def _():
            out[z, :RX] += from_left[i]

        @pl.when(has_right)
        def _():
            out[z, RX:] += from_right[i]

        out[z] *= inverse[...]

    def alone(i):
        return (i < EDGE) | (i >= NZ - EDGE)

    def step(i, now, then):
        @pl.when(i < NZ)
        def _():
            z = NZ - 2 - i

            @pl.when(i + 1 < EDGE)
            def _():
                load(i + 1).wait()

            @pl.when((i + 1 >= EDGE) & (i + 1 < NZ) & ((i + 1) % LOT == 0))
            def _():
                load_lot((i + 1 - EDGE) // LOT).wait()

            along_z(now, then)
            along_y(jnp.maximum(z, 0), then)
            along_x(i, True)
            along_x(i, False)
            start(y_ways, rim, i, 1)

            @pl.when(i == 0)
            def _():
                start(y_ways, ramp_y)

            @pl.when((i % GROUP == GROUP - 1) & (i > HOLD))
            def _():
                start(y_ways, middle, i - HOLD - GROUP + 1, GROUP)

            @pl.when(i == NZ - 1)
            def _():
                for k in range(HOLD, 0, -GROUP):
                    start(y_ways, middle, NZ - k, GROUP)

        ready = i - AHEAD

        @pl.when((ready >= 0) & (ready < NZ))
        def _():
            arrived(y_ways, rim, ready, 1)
            sides(ready)

            @pl.when(alone(ready))
            def _():
                start(x_ways, side, ready, 1)

            @pl.when(jnp.logical_not(alone(ready)) & (ready % 2 == 1))
            def _():
                start(x_ways, side, ready - 1, 2)

            @pl.when(ready == 3)
            def _():
                gather_ramps()

        done = i - BEHIND

        @pl.when((done >= 0) & (done < NZ))
        def _():
            @pl.when(done == 0)
            def _():
                invert()

            @pl.when(done % GROUP == 0)
            def _():
                arrived(y_ways, middle, done, GROUP)

            @pl.when(alone(done))
            def _():
                arrived(x_ways, side, done, 1)

            @pl.when(jnp.logical_not(alone(done)) & (done % 2 == 0))
            def _():
                arrived(x_ways, side, done, 2)

            finish(done)

    def two_steps(pair, carry):
        step(2 * pair, even, odd)
        step(2 * pair + 1, odd, even)
        return carry

    lax.fori_loop(0, (NZ + BEHIND) // 2, two_steps, 0)

    sent(y_ways, ramp_y)
    sent(x_ways, ramp_x)

    sent(y_ways, rim, 0, NZ)
    sent(y_ways, middle, 0, NZ)
    sent(x_ways, side, 0, NZ)


def local(source_tiles, tile_offsets, tile_shifts, tile_counts):
    hbm = pl.BlockSpec(memory_space=pl.ANY)
    dma = pltpu.SemaphoreType.DMA
    volume = pltpu.VMEM((CAP, TX, WY), jnp.float32)
    halo = pltpu.VMEM((NZ, BX, RY), jnp.float32)
    flank = pltpu.VMEM((NZ, RX, BY), jnp.float32)
    ramps = pltpu.VMEM((8, WX + WY), jnp.float32)
    around = pltpu.VMEM((24, WX + BY), jnp.float32)
    return pl.pallas_call(
        kernel,
        out_shape=pltpu.VMEM((NZ, BX, BY), jnp.float32),
        in_specs=[hbm, hbm, hbm, hbm],
        out_specs=pl.BlockSpec(memory_space=pltpu.VMEM),
        scratch_shapes=[
            pltpu.VMEM((CAP, NZ, TX, TY), jnp.bfloat16),
            halo, halo, halo, halo, halo, halo, halo, halo,
            flank, flank, flank, flank,
            volume, volume,
            pltpu.VMEM((CAP, BLOCKS, RX + TX + RX + 8, 128), jnp.float32),
            pltpu.VMEM((CAP, TY, WY), jnp.bfloat16),
            pltpu.VMEM((CAP, 2, WX, 128), jnp.float32),
            pltpu.VMEM((BX, BY), jnp.float32),
            ramps, ramps, ramps, around, around, around,
            pltpu.SMEM((2, CAP), jnp.int32),
            pltpu.SMEM((CAP,), jnp.int32),
            pltpu.SMEM((1,), jnp.int32),
            dma((3,)), dma((EDGE + LOTS,)), dma((8,)),
            dma((6,)), dma((2, 2 * AHEAD + 2)), dma((2, NZ // GROUP)), dma((2, 2 * EDGE + CENTRE)),
        ],
        compiler_params=pltpu.CompilerParams(
            collective_id=0, has_side_effects=True, vmem_limit_bytes=54 * 1024 * 1024,
        ),
    )(source_tiles, tile_offsets, tile_shifts, tile_counts)


def solution(mesh):
    placed = (
        P(("gx", "gy"), None, None, None),
        P(None, ("gx", "gy")),
        P(("gx", "gy")),
        P(("gx", "gy")),
    )
    return jax.shard_map(
        local, mesh=mesh, in_specs=placed, out_specs=P(None, "gx", "gy"), check_vma=False
    )
```

```python
import jax
import jax.numpy as jnp
from jax import lax
from jax.experimental import pallas as pl
from jax.experimental.pallas import tpu as pltpu
from jax.sharding import PartitionSpec as P

NZ = 32
BX = 128
BY = 256
TX = 192
TY = 384
CAP = 3
RAMP = 32
RX = 64
RY = 128
WX = BX + 2 * RX
WY = BY + 2 * RY
AHEAD = 3
BEHIND = 14
HOLD = 4
GROUP = 4
EDGE = 4
LOT = 4
LOTS = (NZ - EDGE) // LOT
CENTRE = (NZ - 2 * EDGE) // 2
ROWS = 16
BLOCKS = WY // 128
MESH = pl.DeviceIdType.MESH


def ramp(places, length):
    return jnp.minimum(jnp.minimum(places + 1, length - places), RAMP)


def taps(places, length, fraction):
    inside = (places >= 0) & (places < length)
    blend = jnp.where(inside, ramp(places, length), 0).astype(jnp.float32)
    last = jnp.where(places == length - 1, fraction, 0.0)
    return blend, blend * (1.0 - fraction + last), blend * fraction


def kernel(
    tiles, offsets_hbm, shifts_hbm, counts_hbm, out,
    source, low_rim, high_rim, low_mid, high_mid,
    from_low_rim, from_high_rim, from_low_mid, from_high_mid,
    left, right, from_left, from_right,
    even, odd, placed, spread_y, spread_x, inverse,
    ramps, ramps_from_low, ramps_from_high, around, around_left, around_right,
    offsets, shifts, counts, number_sem, load_sem, ramp_sem, send_sem, recv_rim, recv_mid, recv_side,
):
    gx = lax.axis_index("gx")
    gy = lax.axis_index("gy")
    has_low, has_high = gy > 0, gy < lax.axis_size("gy") - 1
    has_left, has_right = gx > 0, gx < lax.axis_size("gx") - 1
    below, above = {"gy": gy - 1}, {"gy": gy + 1}
    before, after = {"gx": gx - 1}, {"gx": gx + 1}

    def load(i):
        z = NZ - 1 - i
        return pltpu.make_async_copy(tiles.at[:, z], source.at[:, z], load_sem.at[i])

    def load_lot(lot):
        span = pl.ds(NZ - EDGE - LOT * (lot + 1), LOT)
        return pltpu.make_async_copy(
            tiles.at[:, span], source.at[:, span], load_sem.at[EDGE + lot]
        )

    def remote(src, dst, send, recv, place):
        return pltpu.make_async_remote_copy(
            src_ref=src, dst_ref=dst, send_sem=send, recv_sem=recv,
            device_id=place, device_id_type=MESH,
        )

    def rim(way, z, count):
        src, dst, place = (
            (low_rim, from_high_rim, below), (high_rim, from_low_rim, above)
        )[way]
        span = pl.ds(z, count)
        return remote(
            src.at[span], dst.at[span], send_sem.at[way], recv_rim.at[way, z % (2 * AHEAD + 2)], place
        )

    def middle(way, z, count):
        src, dst, place = (
            (low_mid, from_high_mid, below), (high_mid, from_low_mid, above)
        )[way]
        span = pl.ds(z, count)
        return remote(
            src.at[span], dst.at[span], send_sem.at[2 + way], recv_mid.at[way, z // GROUP], place
        )

    def side(way, z, count):
        src, dst, place = ((left, from_right, before), (right, from_left, after))[way]
        span = pl.ds(z, count)
        inner = jnp.minimum(jnp.maximum(z - EDGE, 0) // 2, CENTRE)
        last = jnp.maximum(z - NZ + EDGE, 0)
        at = jnp.minimum(z, EDGE) + inner + last
        return remote(
            src.at[span], dst.at[span], send_sem.at[4 + way], recv_side.at[way, at], place
        )

    def ramp_y(way):
        dst, place = ((ramps_from_high, below), (ramps_from_low, above))[way]
        return remote(ramps, dst, ramp_sem.at[way], ramp_sem.at[2 + way], place)

    def ramp_x(way):
        dst, place = ((around_right, before), (around_left, after))[way]
        return remote(around, dst, ramp_sem.at[4 + way], ramp_sem.at[6 + way], place)

    y_ways = ((0, has_low, has_high), (1, has_high, has_low))
    x_ways = ((0, has_left, has_right), (1, has_right, has_left))

    def start(ways, make, *place):
        for way, sends, _ in ways:
            @pl.when(sends)
            def _(way=way):
                make(way, *place).start()

    def sent(ways, make, *place):
        for way, sends, _ in ways:
            @pl.when(sends)
            def _(way=way):
                make(way, *place).wait_send()

    def arrived(ways, make, *place):
        for way, _, receives in ways:
            @pl.when(receives)
            def _(way=way):
                make(way, *place).wait_recv()

    numbers = [
        pltpu.make_async_copy(src, dst, number_sem.at[n])
        for n, (src, dst) in enumerate(
            ((offsets_hbm, offsets), (shifts_hbm, shifts), (counts_hbm, counts))
        )
    ]
    for copy in numbers:
        copy.start()
    for i in range(3):
        load(i).start()

    barrier = pltpu.get_barrier_semaphore()
    neighbours = (
        (has_low, below), (has_high, above), (has_left, before), (has_right, after)
    )
    for present, place in neighbours:
        @pl.when(present)
        def _(place=place):
            pl.semaphore_signal(barrier, inc=1, device_id=place, device_id_type=MESH)

    for copy in numbers:
        copy.wait()
    starts_x, starts_y, parts, used, tops = [], [], [], [], []
    for k in range(CAP):
        code = shifts[k]
        starts_x.append(offsets[0, k] - gx * BX + RX)
        starts_y.append(offsets[1, k] - gy * BY + RY)
        tops.append(jnp.minimum(jnp.maximum(RX - starts_x[k], 0), RX))
        parts.append([
            ((code >> bits) & 3).astype(jnp.float32) * 0.25 for bits in (4, 2, 0)
        ])
        used.append(jnp.where(k < counts[0], 1.0, 0.0).astype(jnp.float32))

    taps_y = [
        taps(lax.broadcasted_iota(jnp.int32, (8, WY), 1) - starts_y[k], TY, parts[k][2])
        for k in range(CAP)
    ]
    for k in range(CAP):
        for r in range(0, TY, 64):
            apart = (
                lax.broadcasted_iota(jnp.int32, (64, WY), 0) + r
                - lax.broadcasted_iota(jnp.int32, (64, WY), 1) + starts_y[k]
            )
            own, following = taps_y[k][1][0:1], taps_y[k][2][0:1]
            spread_y[k, r : r + 64] = jnp.where(
                apart == 0, own, jnp.where(apart == 1, following, 0.0)
            ).astype(jnp.bfloat16)

    for k in range(CAP):
        place = lax.broadcasted_iota(jnp.int32, (WX, 128), 0) - starts_x[k]
        _, own, following = taps(place, TX, parts[k][1])
        spread_x[k, 0] = own * used[k]
        spread_x[k, 1] = following * used[k]
    placed[:, :, :RX] = jnp.zeros((CAP, BLOCKS, RX, 128), jnp.float32)
    placed[:, :, RX + TX :] = jnp.zeros((CAP, BLOCKS, RX + 8, 128), jnp.float32)

    ramps[...] = jnp.zeros_like(ramps)
    for k in range(CAP):
        blend = taps(
            lax.broadcasted_iota(jnp.int32, (8, WX), 1) - starts_x[k], TX, parts[k][1]
        )[0]
        ramps[k : k + 1, :WX] = blend[0:1] * used[k]
        ramps[k : k + 1, WX:] = taps_y[k][0][0:1]

    def along_y(z, *volumes):
        for k in range(CAP):
            rows = jnp.dot(
                source[k, z], spread_y[k], preferred_element_type=jnp.float32
            )
            for volume in volumes:
                volume[k] = rows

    load(0).wait()
    along_y(NZ - 1, even, odd)

    load(3).start()
    for lot in range(LOTS):
        load_lot(lot).start()

    pl.semaphore_wait(
        barrier, sum(present.astype(jnp.int32) for present, _ in neighbours)
    )

    def along_z(now, then):
        for k in range(CAP):
            depth_part = parts[k][0]
            for r in range(0, TX, ROWS):
                volume = (1.0 - depth_part) * now[k, r : r + ROWS] + (
                    depth_part * then[k, r : r + ROWS]
                )
                for n in range(BLOCKS):
                    placed[k, n, RX + r : RX + r + ROWS] = volume[:, n * 128 : (n + 1) * 128]

    def along_x(i, rims):
        for r in range(0, WX, ROWS):
            in_rim = r < RX or r >= RX + BX
            rim_row = r if r < RX else r - BX
            weights = [
                (spread_x[k, 0, r : r + ROWS], spread_x[k, 1, r : r + ROWS])
                for k in range(CAP)
            ]
            for n in range(BLOCKS):
                at_end = n in (0, BLOCKS - 1)
                if rims != (in_rim and at_end):
                    continue
                total = None
                for k in range(CAP):
                    first = tops[k] + r
                    term = weights[k][0] * placed[k, n, pl.ds(first, ROWS)] + (
                        weights[k][1] * placed[k, n, pl.ds(first + 1, ROWS)]
                    )
                    total = term if total is None else total + term
                if rims:
                    (low_rim if n == 0 else high_rim)[i, rim_row : rim_row + ROWS] = total
                elif at_end:
                    (low_mid if n == 0 else high_mid)[i, r - RX : r - RX + ROWS] = total
                else:
                    lanes = slice((n - 1) * 128, n * 128)
                    if r < RX:
                        left[i, r : r + ROWS, lanes] = total
                    elif in_rim:
                        right[i, r - RX - BX : r - RX - BX + ROWS, lanes] = total
                    else:
                        out[NZ - 1 - i, r - RX : r - RX + ROWS, lanes] = total

    def gather_ramps():
        around[...] = jnp.zeros_like(around)
        around[0:8, :WX] = ramps[:, :WX]
        around[0:8, WX:] = ramps[:, WX + RY : WX + RY + BY]
        arrived(y_ways, ramp_y)

        @pl.when(has_low)
        def _():
            around[8:16, :WX] = ramps_from_low[:, :WX]
            around[8:16, WX : WX + RY] = ramps_from_low[:, WX + RY + BY :]

        @pl.when(has_high)
        def _():
            around[16:24, :WX] = ramps_from_high[:, :WX]
            around[16:24, WX + RY :] = ramps_from_high[:, WX : WX + RY]

        start(x_ways, ramp_x)

    def weights_of(rows):
        return lax.dot_general(
            rows[:, :WX].astype(jnp.bfloat16), rows[:, WX:].astype(jnp.bfloat16),
            (((0,), (0,)), ((), ())), preferred_element_type=jnp.float32,
        )

    def invert():
        inverse[...] = weights_of(around[...])[RX : RX + BX]
        arrived(x_ways, ramp_x)

        @pl.when(has_left)
        def _():
            inverse[:RX] += weights_of(around_left[...])[RX + BX :]

        @pl.when(has_right)
        def _():
            inverse[RX:] += weights_of(around_right[...])[:RX]

        inverse[...] = 1.0 / jnp.maximum(inverse[...], 1.0)

    def sides(z):
        @pl.when(has_low)
        def _():
            left[z, :, :RY] += from_low_rim[z, :RX]
            right[z, :, :RY] += from_low_rim[z, RX:]

        @pl.when(has_high)
        def _():
            left[z, :, RY:] += from_high_rim[z, :RX]
            right[z, :, RY:] += from_high_rim[z, RX:]

    def finish(i):
        z = NZ - 1 - i

        inner = has_low & has_high & has_left & has_right

        @pl.when(inner)
        def _():
            for rows, flank in ((slice(0, RX), from_left), (slice(RX, BX), from_right)):
                for lanes, halo in (
                    (slice(0, RY), from_low_mid), (slice(RY, BY), from_high_mid)
                ):
                    out[z, rows, lanes] = (
                        out[z, rows, lanes] + halo[i, rows] + flank[i, :, lanes]
                    ) * inverse[rows, lanes]

        @pl.when(jnp.logical_not(inner))
        def _():
            @pl.when(has_low)
            def _():
                out[z, :, :RY] += from_low_mid[i]

            @pl.when(has_high)
            def _():
                out[z, :, RY:] += from_high_mid[i]

            @pl.when(has_left)
            def _():
                out[z, :RX] += from_left[i]

            @pl.when(has_right)
            def _():
                out[z, RX:] += from_right[i]

            out[z] *= inverse[...]

    def alone(i):
        return (i < EDGE) | (i >= NZ - EDGE)

    def step(i, now, then):
        @pl.when(i < NZ)
        def _():
            z = NZ - 2 - i

            @pl.when(i + 1 < EDGE)
            def _():
                load(i + 1).wait()

            @pl.when((i + 1 >= EDGE) & (i + 1 < NZ) & ((i + 1) % LOT == 0))
            def _():
                load_lot((i + 1 - EDGE) // LOT).wait()

            along_z(now, then)
            along_x(i, True)
            along_y(jnp.maximum(z, 0), then)
            along_x(i, False)
            start(y_ways, rim, i, 1)

            @pl.when(i == 0)
            def _():
                start(y_ways, ramp_y)

            @pl.when((i % GROUP == GROUP - 1) & (i > HOLD))
            def _():
                start(y_ways, middle, i - HOLD - GROUP + 1, GROUP)

            @pl.when(i == NZ - 1)
            def _():
                for k in range(HOLD, 0, -GROUP):
                    start(y_ways, middle, NZ - k, GROUP)

        ready = i - AHEAD

        @pl.when((ready >= 0) & (ready < NZ))
        def _():
            arrived(y_ways, rim, ready, 1)
            sides(ready)

            @pl.when(alone(ready))
            def _():
                start(x_ways, side, ready, 1)

            @pl.when(jnp.logical_not(alone(ready)) & (ready % 2 == 1))
            def _():
                start(x_ways, side, ready - 1, 2)

            @pl.when(ready == 3)
            def _():
                gather_ramps()

        done = i - BEHIND

        @pl.when((done >= 0) & (done < NZ))
        def _():
            @pl.when(done == 0)
            def _():
                invert()

            @pl.when(done % GROUP == 0)
            def _():
                arrived(y_ways, middle, done, GROUP)

            @pl.when(alone(done))
            def _():
                arrived(x_ways, side, done, 1)

            @pl.when(jnp.logical_not(alone(done)) & (done % 2 == 0))
            def _():
                arrived(x_ways, side, done, 2)

            finish(done)

    def two_steps(pair, carry):
        step(2 * pair, even, odd)
        step(2 * pair + 1, odd, even)
        return carry

    lax.fori_loop(0, (NZ + BEHIND) // 2, two_steps, 0)

    sent(y_ways, ramp_y)
    sent(x_ways, ramp_x)

    sent(y_ways, rim, 0, NZ)
    sent(y_ways, middle, 0, NZ)
    sent(x_ways, side, 0, NZ)


def local(source_tiles, tile_offsets, tile_shifts, tile_counts):
    hbm = pl.BlockSpec(memory_space=pl.ANY)
    dma = pltpu.SemaphoreType.DMA
    volume = pltpu.VMEM((CAP, TX, WY), jnp.float32)
    halo = pltpu.VMEM((NZ, BX, RY), jnp.float32)
    flank = pltpu.VMEM((NZ, RX, BY), jnp.float32)
    ramps = pltpu.VMEM((8, WX + WY), jnp.float32)
    around = pltpu.VMEM((24, WX + BY), jnp.float32)
    return pl.pallas_call(
        kernel,
        out_shape=pltpu.VMEM((NZ, BX, BY), jnp.float32),
        in_specs=[hbm, hbm, hbm, hbm],
        out_specs=pl.BlockSpec(memory_space=pltpu.VMEM),
        scratch_shapes=[
            pltpu.VMEM((CAP, NZ, TX, TY), jnp.bfloat16),
            halo, halo, halo, halo, halo, halo, halo, halo,
            flank, flank, flank, flank,
            volume, volume,
            pltpu.VMEM((CAP, BLOCKS, RX + TX + RX + 8, 128), jnp.float32),
            pltpu.VMEM((CAP, TY, WY), jnp.bfloat16),
            pltpu.VMEM((CAP, 2, WX, 128), jnp.float32),
            pltpu.VMEM((BX, BY), jnp.float32),
            ramps, ramps, ramps, around, around, around,
            pltpu.SMEM((2, CAP), jnp.int32),
            pltpu.SMEM((CAP,), jnp.int32),
            pltpu.SMEM((1,), jnp.int32),
            dma((3,)), dma((EDGE + LOTS,)), dma((8,)),
            dma((6,)), dma((2, 2 * AHEAD + 2)), dma((2, NZ // GROUP)), dma((2, 2 * EDGE + CENTRE)),
        ],
        compiler_params=pltpu.CompilerParams(
            collective_id=0, has_side_effects=True, vmem_limit_bytes=54 * 1024 * 1024,
        ),
    )(source_tiles, tile_offsets, tile_shifts, tile_counts)


def solution(mesh):
    placed = (
        P(("gx", "gy"), None, None, None),
        P(None, ("gx", "gy")),
        P(("gx", "gy")),
        P(("gx", "gy")),
    )
    return jax.shard_map(
        local, mesh=mesh, in_specs=placed, out_specs=P(None, "gx", "gy"), check_vma=False
    )
```
